32 devices in a mesh: rep: 4 (over x, y), dp: 8 (over z, core).
Axes of the slice: x: 2, y: 2, z: 4, core: 2. Of those that a mesh axis runs over, the one named last changes fastest.
Arguments:
- x: bfloat16 [32, 2048, 1024], P(('rep', 'dp')), parts along dimension 0
- dy: bfloat16 [32, 2048, 1024], P(('rep', 'dp')), parts along dimension 0
- w_gate: bfloat16 [2, 1024, 4096], replicated
- w_up: bfloat16 [2, 1024, 4096], replicated
- w_down: bfloat16 [2, 4096, 1024], replicated
- m_w_gate: float32 [2, 1024, 4096], P(None, 'dp')
- m_w_up: float32 [2, 1024, 4096], P(None, 'dp')
- m_w_down: float32 [2, 4096, 1024], P(None, 'dp')
- v_w_gate: float32 [2, 1024, 4096], P(None, 'dp')
- v_w_up: float32 [2, 1024, 4096], P(None, 'dp')
- v_w_down: float32 [2, 4096, 1024], P(None, 'dp')
Outputs:
- output 1: bfloat16 [8, 1024, 4096], P('rep'), parts along dimension 0
- output 2: bfloat16 [8, 1024, 4096], P('rep'), parts along dimension 0
- output 3: bfloat16 [8, 4096, 1024], P('rep'), parts along dimension 0
- output 4: float32 [8, 1024, 4096], P('rep', 'dp'), parts along dimension 0
- output 5: float32 [8, 1024, 4096], P('rep', 'dp'), parts along dimension 0
- output 6: float32 [8, 4096, 1024], P('rep', 'dp'), parts along dimension 0
- output 7: float32 [8, 1024, 4096], P('rep', 'dp'), parts along dimension 0
- output 8: float32 [8, 1024, 4096], P('rep', 'dp'), parts along dimension 0
- output 9: float32 [8, 4096, 1024], P('rep', 'dp'), parts along dimension 0
There are 4 independent parts. The reference program is written for one: setup_inputs(seed, part) draws one part's arguments, and reference() takes and returns one part's arrays. A program takes and returns all parts, laid end to end along the dimension named above; an argument that names none is the same for every part.
All inputs are finite; a program needn't handle non-finite values.
Results may differ from the reference program's by a relative error of at most 0.022.
Values are sent between devices in bfloat16 or wider.
A program may use at most 2 GiB of HBM per device.

```python
import jax
import jax.numpy as jnp
from jax import lax

SEQUENCES = 8
TOKENS = 2048
D = 1024
FF = 4096
LAYERS = 2
NAMES = ("w_gate", "w_up", "w_down")
SHAPES = {"w_gate": (LAYERS, D, FF), "w_up": (LAYERS, D, FF), "w_down": (LAYERS, FF, D)}


def bump(key, n, height):
    away = (jnp.arange(n, dtype=jnp.int32) - jax.random.randint(key, (), 0, n, jnp.int32)) % n
    return jnp.where(away < n // 8, height, 1.0)


def together(key, own, strength):
    shared = jax.random.normal(key, own.shape[1:], jnp.float32)
    return (own + strength * shared) * lax.rsqrt(1 + strength * strength)


def setup_inputs(seed: int = 0, part: int = 0) -> dict:
    kx, kdy, ka, kb, kz, kf, kh, kl, *keys = jax.random.split(jax.random.key(seed), 8 + 3 * len(NAMES))
    kx, kdy, ka, kb = (jax.random.fold_in(k, part) for k in (kx, kdy, ka, kb))
    kw, km, kv = (keys[i::3] for i in range(3))
    shape = (SEQUENCES, TOKENS, D)
    much_x, much_dy = jax.random.uniform(kz, (2,), jnp.float32, 0.0, 1.0)
    loud = 2.0 ** jax.random.uniform(jax.random.fold_in(kz, 1), (), jnp.float32, -1.0, 2.0)
    layers = 2.0 ** jax.random.uniform(kl, (LAYERS, 1, 1), jnp.float32, -1.0, 1.0)
    x = together(ka, jax.random.normal(kx, shape, jnp.float32), much_x) * bump(kf, D, 4.0)
    dy = together(kb, jax.random.normal(kdy, shape, jnp.float32), much_dy)
    drawn = {"x": x.astype(jnp.bfloat16), "dy": (loud * dy * (SEQUENCES * TOKENS) ** -0.5).astype(jnp.bfloat16)}
    for key, name in zip(kw, NAMES, strict=True):
        w = jax.random.normal(key, SHAPES[name], jnp.float32) * SHAPES[name][1] ** -0.5
        drawn[name] = (w * {"w_gate": 1.0, "w_up": bump(kh, FF, 4.0), "w_down": layers}[name]).astype(jnp.bfloat16)
    for key, name in zip(km, NAMES, strict=True):
        drawn[f"m_{name}"] = 0.1 * jax.random.normal(key, SHAPES[name], jnp.float32)
    for key, name in zip(kv, NAMES, strict=True):
        drawn[f"v_{name}"] = jax.random.uniform(key, SHAPES[name], jnp.float32, 0.005, 0.015)
    return drawn


def matmul(a, w):
    return jnp.dot(a, w, preferred_element_type=jnp.float32).astype(jnp.bfloat16)


def normed(h):
    wide = h.astype(jnp.float32)
    scale = lax.rsqrt(jnp.mean(wide**2, -1, keepdims=True) + 1e-6)
    return (wide * scale).astype(jnp.bfloat16)


def layer(h, w):
    a = normed(h)
    gate = jnp.dot(a, w["w_gate"], preferred_element_type=jnp.float32)
    up = jnp.dot(a, w["w_up"], preferred_element_type=jnp.float32)
    return h + matmul((jax.nn.silu(gate) * up).astype(jnp.bfloat16), w["w_down"])


def adamw(w, m, v, g):
    m = 0.9 * m + 0.1 * g
    v = 0.95 * v + 0.05 * g * g
    step = m * lax.rsqrt(v + 1e-8) + 0.1 * w
    return (w - 0.02 * step).astype(jnp.bfloat16), m, v


def stack(weights, h):
    return lax.scan(lambda h, w: (layer(h, w), None), h, weights)[0]


def reference(x, dy, w_gate, w_up, w_down, m_w_gate, m_w_up, m_w_down, v_w_gate, v_w_up, v_w_down):
    weights = dict(zip(NAMES, (w_gate, w_up, w_down), strict=True))

    def take(so_far, sequence):
        h, by_y = sequence
        _, back = jax.vjp(lambda w: stack(w, h), weights)
        return jax.tree.map(lambda total, term: total + term.astype(jnp.float32), so_far, back(by_y)[0]), None

    none_yet = {name: jnp.zeros(w.shape, jnp.float32) for name, w in weights.items()}
    by_weights, _ = lax.scan(take, none_yet, (x, dy))
    gradients = [by_weights[name].astype(jnp.bfloat16).astype(jnp.float32) for name in NAMES]
    new = [
        adamw(w.astype(jnp.float32), m, v, g)
        for w, m, v, g in zip((w_gate, w_up, w_down), (m_w_gate, m_w_up, m_w_down), (v_w_gate, v_w_up, v_w_down), gradients, strict=True)
    ]
    return tuple(one[which] for which in range(3) for one in new)
```

```python
import functools

import jax
import jax.numpy as jnp
from jax import lax
from jax.experimental import pallas as pl
from jax.experimental.pallas import tpu as pltpu
from jax.sharding import PartitionSpec as P

MESH = pl.DeviceIdType.MESH
T, D, FF = 2048, 1024, 4096
CHIPS = 4
OWNERS = 8
W = 128
TILE = 1024
UNITS = 24
STEPS = 24
TILES = 8
VMEM_LIMIT = 63 << 20
WAYS = (0, 1)
ALONG = ((1,), (1,))
F32, BF16 = jnp.float32, jnp.bfloat16


def normed(wide):
    return (wide * lax.rsqrt(jnp.mean(wide * wide, -1, keepdims=True) + 1e-6)).astype(BF16)


def dot(a, b, dims=((1,), (0,))):
    return lax.dot_general(a, b, (dims, ((), ())), preferred_element_type=F32)


def main(
    x_hbm, dy_hbm, wg_hbm, wu_hbm, wd_hbm, mg_hbm, mu_hbm, md_hbm, vg_hbm, vu_hbm, vd_hbm,
    st, mo, vo, own, par, in_r, in_l, h_hbm,
    a_v, at_v, dy_v, wg_v, wu_v, wd_v, actt_v, dg_v, du_v, da_v, stage,
    t_own, t_par, t_in, t_out, f_own, f_par, f_r, f_l, f_m, f_v, f_w, n_w, n_m, n_v,
    w_sem, big_sem, h_sem, stage_sem, par_sem, t_sem, out_sem, rs_sem, f_sem, n_sem, ag_sem, fwd_sem, d_send, d_recv,
):
    me = lax.axis_index("dp")
    z, core = lax.div(me, 2), lax.rem(me, 2)
    partner = me + 1 - 2 * core
    ends = (3 - z, z)
    behind = (z, 3 - z)
    ahead = (me + 2, me - 2)
    incoming = (in_r, in_l)
    copy = pltpu.make_async_copy

    def remote(src, dst, send, recv, to):
        return pltpu.make_async_remote_copy(
            src_ref=src, dst_ref=dst, send_sem=send, recv_sem=recv, device_id={"dp": to}, device_id_type=MESH
        )

    barrier = pltpu.get_barrier_semaphore()
    pl.semaphore_signal(barrier, inc=1, device_id={"dp": partner}, device_id_type=MESH)
    for way in WAYS:

        @pl.when(ends[way] >= 1)
        def _():
            pl.semaphore_signal(barrier, inc=1, device_id={"dp": ahead[way]}, device_id_type=MESH)

    def strips(src, dst, sem, row, rows, layer, tile):
        for i in range(OWNERS):
            copy(
                src.at[layer, pl.ds(row, rows), pl.ds(pl.multiple_of(512 * i + W * tile, W), W)],
                dst.at[:, pl.ds(W * i, W)],
                sem,
            ).start()

    def weights_in(layer, tile, slot=0):
        strips(wg_hbm, wg_v.at[slot], w_sem.at[slot, 0], 0, D, layer, tile)
        strips(wu_hbm, wu_v.at[slot], w_sem.at[slot, 1], 0, D, layer, tile)

    def down_in(layer, tile, slot=0):
        for i in range(OWNERS):
            copy(
                wd_hbm.at[layer, pl.ds(pl.multiple_of(512 * i + W * tile, W), W), :],
                wd_v.at[slot, pl.ds(W * i, W), :],
                w_sem.at[slot, 2],
            ).start()

    def weights_wait(slot=0):
        for number, w in enumerate((wg_v, wu_v, wd_v)):
            copy(w.at[slot], w.at[slot], w_sem.at[slot, number]).wait()


    def at_block(i):
        return pl.ds(pl.multiple_of(i * W, W), W)

    def live(u):
        return (u >= 0) & (u < UNITS)

    def sends(way, hop, u):
        return live(u) & (behind[way] <= hop - 1) & (ends[way] >= 1)

    def sum_begin(u, hop):
        for way in WAYS:
            block = z + 4 - hop if way == 0 else z + hop - 4

            @pl.when(sends(way, hop, u))
            def _():
                copy(own.at[u, block], t_own.at[way], t_sem.at[way, 0]).start()
                copy(par.at[u, block], t_par.at[way], t_sem.at[way, 1]).start()

            if hop > 1:

                @pl.when(sends(way, hop, u) & (behind[way] >= 1))
                def _():
                    landed = incoming[way].at[u, hop - 2]
                    remote(landed, landed, out_sem.at[way, hop - 1], rs_sem.at[way, u, hop - 2], partner).wait_recv()
                    copy(landed, t_in.at[way], t_sem.at[way, 2]).start()

    def sum_out(way, hop, u):
        return remote(
            t_out.at[way, hop - 1],
            incoming[way].at[u, hop - 1],
            out_sem.at[way, hop - 1],
            rs_sem.at[way, u, hop - 1],
            ahead[way],
        )

    def sum_finish(u, hop):
        for way in WAYS:

            @pl.when(sends(way, hop, u) & (u >= 1))
            def _():
                sum_out(way, hop, u - 1).wait_send()

            @pl.when(sends(way, hop, u))
            def _():
                copy(own.at[u, 0], t_own.at[way], t_sem.at[way, 0]).wait()
                copy(par.at[u, 0], t_par.at[way], t_sem.at[way, 1]).wait()

                @pl.when(behind[way] == 0)
                def _():
                    t_out[way, hop - 1] = (t_own[way].astype(F32) + t_par[way].astype(F32)).astype(BF16)

                if hop > 1:

                    @pl.when(behind[way] >= 1)
                    def _():
                        copy(own.at[u, 0], t_in.at[way], t_sem.at[way, 2]).wait()
                        t_out[way, hop - 1] = (
                            t_own[way].astype(F32) + t_par[way].astype(F32) + t_in[way].astype(F32)
                        ).astype(BF16)

                sum_out(way, hop, u).start()

    def kind(u):
        tile = lax.div(u, 3)
        return lax.rem(u, 3), 1 - lax.div(tile, 4), lax.rem(tile, 4)

    def step_begin(u):
        @pl.when(live(u))
        def _():
            copy(own.at[u, z], f_own, f_sem.at[0]).start()
            copy(par.at[u, z], f_par, f_sem.at[1]).start()
            matrix, layer, tile = kind(u)

            @pl.when(matrix == 0)
            def _():
                copy(md_hbm.at[layer, at_block(tile), :], f_m, f_sem.at[4]).start()
                copy(vd_hbm.at[layer, at_block(tile), :], f_v, f_sem.at[5]).start()
                row = pl.ds(pl.multiple_of(512 * me + W * tile, W), W)
                copy(wd_hbm.at[layer, row, :], f_w, f_sem.at[6]).start()

            for number, (m, v, w) in enumerate(((mg_hbm, vg_hbm, wg_hbm), (mu_hbm, vu_hbm, wu_hbm))):

                @pl.when(matrix == number + 1)
                def _():
                    strips(m, f_m, f_sem.at[4], 0, W, layer, tile)
                    strips(v, f_v, f_sem.at[5], 0, W, layer, tile)
                    strips(w, f_w, f_sem.at[6], pl.multiple_of(W * me, W), W, layer, tile)

            for way, f_in in enumerate((f_r, f_l)):

                @pl.when(behind[way] >= 1)
                def _():
                    landed = incoming[way].at[u, 2]
                    remote(landed, landed, out_sem.at[way, 2], rs_sem.at[way, u, 2], partner).wait_recv()
                    copy(landed, f_in, f_sem.at[2 + way]).start()

    def results(u):
        slot = lax.rem(u + 2, 2)
        here = st.at[u, me]
        for way in WAYS:
            yield ends[way] >= 1, remote(n_w.at[slot], here, n_sem.at[slot, way], ag_sem.at[way, u, 0], ahead[way])
        yield None, remote(n_w.at[slot], here, n_sem.at[slot, 2], d_recv.at[u], partner)
        yield None, copy(n_w.at[slot], here, n_sem.at[slot, 3])
        yield None, copy(n_m.at[slot], mo.at[u], n_sem.at[slot, 4])
        yield None, copy(n_v.at[slot], vo.at[u], n_sem.at[slot, 5])

    def results_start(u):
        for condition, c in results(u):
            if condition is None:
                c.start()
            else:
                pl.when(condition)(c.start)

    def results_wait(u):
        for number, (condition, c) in enumerate(results(u)):
            wait = c.wait_send if number < 3 else c.wait
            if condition is None:
                wait()
            else:
                pl.when(condition)(wait)

    def step_finish(u):
        @pl.when(live(u) & (u >= 2))
        def _():
            results_wait(u - 2)

        @pl.when(live(u))
        def _():
            slot = lax.rem(u + 2, 2)
            copy(own.at[u, 0], f_own, f_sem.at[0]).wait()
            copy(par.at[u, 0], f_par, f_sem.at[1]).wait()
            copy(mo.at[u], f_m, f_sem.at[4]).wait()
            copy(vo.at[u], f_v, f_sem.at[5]).wait()
            copy(own.at[u, 0], f_w, f_sem.at[6]).wait()
            for way, f_in in enumerate((f_r, f_l)):

                @pl.when(behind[way] >= 1)
                def _():
                    copy(own.at[u, 0], f_in, f_sem.at[2 + way]).wait()

            def update(rows, incoming_sum):
                g = f_own[rows, :].astype(F32) + f_par[rows, :].astype(F32) + incoming_sum
                g = g.astype(BF16).astype(F32)
                m = 0.9 * f_m[rows, :] + 0.1 * g
                v = 0.95 * f_v[rows, :] + 0.05 * g * g
                w = f_w[rows, :].astype(F32)
                n_m[slot, rows, :] = m
                n_v[slot, rows, :] = v
                n_w[slot, rows, :] = (w - 0.02 * (m * lax.rsqrt(v + 1e-8) + 0.1 * w)).astype(BF16)

            def updates(*incoming_sums):
                @pl.loop(0, W // 32)
                def _(r):
                    rows = pl.ds(pl.multiple_of(r * 32, 32), 32)
                    update(rows, sum(one[rows, :].astype(F32) for one in incoming_sums))

            pl.when(z == 0)(functools.partial(updates, f_l))
            pl.when(z == CHIPS - 1)(functools.partial(updates, f_r))
            pl.when((z > 0) & (z < CHIPS - 1))(functools.partial(updates, f_r, f_l))
            results_start(u)

    def gathered(way, hop, u):
        return st.at[u, me - 2 * (hop - 1) if way == 0 else me + 2 * (hop - 1)]

    def pass_on(way, hop, u):
        block = gathered(way, hop, u)
        return remote(block, block, fwd_sem.at[way, hop - 2], ag_sem.at[way, u, hop - 1], ahead[way])

    def across(way, hop, u):
        block = gathered(way, hop, u)
        return remote(block, block, d_send.at[way, hop - 2], d_recv.at[u], partner)

    def gather(u, hop):
        for way in WAYS:

            @pl.when(live(u) & (behind[way] >= hop - 1))
            def _():
                block = gathered(way, hop, u)
                remote(block, block, d_send.at[way, hop - 2], ag_sem.at[way, u, hop - 2], partner).wait_recv()
                if hop < 4:

                    @pl.when((ends[way] >= 1) & (u >= 1))
                    def _():
                        pass_on(way, hop, u - 1).wait_send()

                    @pl.when(ends[way] >= 1)
                    def _():
                        pass_on(way, hop, u).start()

                @pl.when(u >= 1)
                def _():
                    across(way, hop, u - 1).wait_send()

                across(way, hop, u).start()

    def links(n):
        j, phase = lax.div(n, 8), lax.rem(n, 8)

        @pl.when(phase == 0)
        def _():
            @pl.when(live(j))
            def _():
                remote(own.at[j], par.at[j], stage_sem.at[0, 1], par_sem.at[j], partner).wait_recv()

            sum_begin(j, 1)
            gather(j - 3, 2)

        @pl.when(phase == 1)
        def _():
            sum_finish(j, 1)

        @pl.when(phase == 2)
        def _():
            step_begin(j - 2)

        @pl.when(phase == 3)
        def _():
            step_finish(j - 2)

        @pl.when(phase == 4)
        def _():
            sum_begin(j - 1, 3)
            gather(j - 4, 4)

        @pl.when(phase == 5)
        def _():
            sum_finish(j - 1, 3)

        @pl.when(phase == 6)
        def _():
            sum_begin(j, 2)
            gather(j - 3, 3)

        @pl.when(phase == 7)
        def _():
            sum_finish(j, 2)


    def stage_copies(n):
        slot, u, q = lax.rem(n, 2), lax.div(n, 4), lax.rem(n, 4)
        stay = copy(stage.at[slot, at_block(core), :], own.at[u, q], stage_sem.at[slot, 0])
        go = remote(stage.at[slot, at_block(1 - core), :], par.at[u, q], stage_sem.at[slot, 1], par_sem.at[u], partner)
        return stay, go

    def stage_wait(n):
        stay, go = stage_copies(n)
        stay.wait()
        go.wait_send()

    def gradient(tile, matrix, q, left, right):
        n = (3 * tile + matrix) * 4 + q
        rows = pl.ds(pl.multiple_of(q * 256, 256), 256)
        stage[lax.rem(n, 2)] = dot(left[rows, :], right[...]).astype(BF16)
        for c in stage_copies(n):
            c.start()

    def chunk(k, rows=512):
        return pl.ds(pl.multiple_of(k * rows, rows), rows)

    half = T // 2

    def x_in(c):
        return copy(x_hbm.at[chunk(c, half), :], du_v.at[chunk(c, half), :], h_sem.at[c])

    def h_out(c):
        return copy(du_v.at[chunk(c, half), :], h_hbm.at[chunk(c, half), :], h_sem.at[c])

    for c in (0, 1):
        x_in(c).start()
    weights_in(0, 0)
    down_in(0, 0)
    copy(dy_hbm, dy_v, big_sem.at[1]).start()

    def forward(t, carry):
        tile, c = lax.div(t, 2), lax.rem(t, 2)
        slot = lax.rem(tile, 2)

        @pl.when(tile == 0)
        def _():
            x_in(c).wait()

            @pl.loop(0, 8)
            def _(r):
                rows = pl.ds(pl.multiple_of(c * half + r * W, W), W)
                a_v[rows, :] = normed(du_v[rows, :].astype(F32))

        @pl.when(c == 0)
        def _():
            weights_wait(slot)
            ahead = lax.div(tile + 1, 4), lax.rem(tile + 1, 4), 1 - slot
            weights_in(*ahead)
            down_in(*ahead)

        rows = chunk(c, half)
        for n in range(4):
            cols = pl.ds(256 * n, 256)
            a = a_v[rows, :]
            gate = dot(a, wg_v[slot, :, cols])
            up = dot(a, wu_v[slot, :, cols])
            dg_v[rows, cols] = (gate * jax.nn.sigmoid(gate) * up).astype(BF16)
        more = dot(dg_v[rows, :], wd_v[slot])

        @pl.when(tile == 0)
        def _():
            da_v[rows, :] = more

        @pl.when(tile > 0)
        def _():
            da_v[rows, :] += more

        @pl.when(tile == 3)
        def _():
            @pl.loop(0, 8)
            def _(r):
                rows = pl.ds(pl.multiple_of(c * half + r * W, W), W)
                h = (du_v[rows, :].astype(F32) + da_v[rows, :].astype(BF16).astype(F32)).astype(BF16)
                du_v[rows, :] = h
                a_v[rows, :] = normed(h.astype(F32))

            h_out(c).start()

        return carry

    lax.fori_loop(0, 8, forward, 0)

    def hidden(rows, cols):
        a = a_v[rows, :]
        gate = dot(a, wg_v[0, :, cols])
        up = dot(a, wu_v[0, :, cols])
        back = dot(dy_v[rows, :], wd_v[0, cols, :], ALONG).astype(BF16).astype(F32)
        sig = jax.nn.sigmoid(gate)
        silu = gate * sig
        actt_v[cols, rows] = (silu * up).astype(BF16).T
        du_v[rows, cols] = (back * silu).astype(BF16)
        dg_v[rows, cols] = (back * up * (sig * (1.0 + gate * (1.0 - sig)))).astype(BF16)

    weights_wait()
    copy(dy_hbm, dy_v, big_sem.at[1]).wait()

    def first(c, carry):
        h_out(c).wait()
        for n in range(4):
            hidden(chunk(c, half), pl.ds(256 * n, 256))
        return carry

    lax.fori_loop(0, 2, first, 0)
    pl.semaphore_wait(barrier, 1 + (z > 0).astype(jnp.int32) + (z < 3).astype(jnp.int32))

    def body(t, carry):
        tile, k = lax.div(t, STEPS), lax.rem(t, STEPS)
        top = tile < 4

        pl.when(k == 0)(weights_wait)

        @pl.when((k == 0) & (tile == 4))
        def _():
            copy(x_hbm, a_v, big_sem.at[0]).wait()

            @pl.loop(0, 8)
            def _(c):
                a_v[chunk(c, 256), :] = normed(a_v[chunk(c, 256), :].astype(F32))

        @pl.when(k < 8)
        def _():
            hidden(chunk(lax.div(k, 2)), chunk(lax.rem(k, 2)))

        @pl.when((k == 8) & (tile < 7))
        def _():
            down_in(1 - lax.div(tile + 1, 4), lax.rem(tile + 1, 4))

        @pl.when((k == 8) & (tile == 3))
        def _():
            copy(h_hbm, a_v, big_sem.at[0]).start()

        @pl.when((k >= 8) & (k < 12))
        def _():
            gradient(tile, 0, k - 8, actt_v, dy_v)

        @pl.when((k >= 12) & (k < 16) & (lax.rem(tile, 4) == 0))
        def _():
            rows = chunk(k - 12)
            at_v[:, rows] = a_v[rows, :].T

        @pl.when((k >= 12) & (k < 16) & top)
        def _():
            rows = chunk(k - 12)
            more = dot(dg_v[rows, :], wg_v[0], ALONG) + dot(du_v[rows, :], wu_v[0], ALONG)

            @pl.when(tile == 0)
            def _():
                da_v[rows, :] = more

            @pl.when(tile > 0)
            def _():
                da_v[rows, :] += more

        @pl.when((k == 12) & (tile == 3))
        def _():
            copy(h_hbm, a_v, big_sem.at[0]).wait()

        @pl.when((k >= 12) & (k < 16) & (tile == 3))
        def _():
            @pl.loop(0, 4)
            def _(r):
                rows = pl.ds(pl.multiple_of((k - 12) * 512 + r * 128, 128), 128)
                wide = a_v[rows, :].astype(F32)
                da = da_v[rows, :].astype(BF16).astype(F32)
                scale = lax.rsqrt(jnp.mean(wide * wide, -1, keepdims=True) + 1e-6)
                along = jnp.sum(da * wide, -1, keepdims=True) * (scale * scale * scale) * (1.0 / D)
                dh = (da * scale - wide * along).astype(BF16)
                dy_v[rows, :] = (dy_v[rows, :].astype(F32) + dh.astype(F32)).astype(BF16)

        @pl.when((k == 16) & (tile < 7))
        def _():
            weights_in(1 - lax.div(tile + 1, 4), lax.rem(tile + 1, 4))

        @pl.when((k == 16) & (tile == 3))
        def _():
            copy(x_hbm, a_v, big_sem.at[0]).start()

        @pl.when((k >= 16) & (k < 20))
        def _():
            gradient(tile, 1, k - 16, at_v, dg_v)

        @pl.when(k >= 20)
        def _():
            gradient(tile, 2, k - 20, at_v, du_v)

        @pl.when((k >= 9) & (k < 13))
        def _():
            stage_wait(12 * tile + k - 9)

        @pl.when(k >= 17)
        def _():
            stage_wait(12 * tile + 4 + k - 17)

        @pl.when((k == 0) & (tile > 0))
        def _():
            stage_wait(12 * tile - 1)

        @pl.when(t >= 12)
        def _():
            links(t - 12)

        return carry

    lax.fori_loop(8, TILES * STEPS, body, 0)
    stage_wait(4 * UNITS - 1)

    def rest(n, carry):
        links(n)
        return carry

    lax.fori_loop(TILES * STEPS - 12, 27 * 8 + 5, rest, 0)

    last = UNITS - 1
    for way in WAYS:
        for hop in (1, 2, 3):
            pl.when(sends(way, hop, last))(sum_out(way, hop, last).wait_send)
        for hop in (2, 3, 4):

            @pl.when(behind[way] >= hop - 1)
            def _():
                if hop < 4:
                    pl.when(ends[way] >= 1)(pass_on(way, hop, last).wait_send)
                across(way, hop, last).wait_send()

    results_wait(last - 1)
    results_wait(last)

    def arrived(u, carry):
        remote(own.at[u], par.at[u], d_send.at[0, 0], d_recv.at[u], partner).wait_recv()
        return carry

    lax.fori_loop(0, UNITS, arrived, 0)


def run_main(*args):
    like = jax.ShapeDtypeStruct
    any_spec = pl.BlockSpec(memory_space=pl.ANY)
    block = (W, D)
    outs = [(OWNERS, BF16), (1, F32), (1, F32), (CHIPS, BF16), (CHIPS, BF16), (3, BF16), (3, BF16)]
    wide, deep, blocks, pair = (T, D), (D, T), (2, *block), (2, 3)
    scratch = [(wide, BF16), (deep, BF16), (wide, BF16), *[((2, D, TILE), BF16)] * 3, (deep, BF16), *[(wide, BF16)] * 2, (wide, F32)]
    scratch += [((2, 256, D), BF16), *[(blocks, BF16)] * 3, ((2, 3, *block), BF16), *[(block, BF16)] * 4, *[(block, F32)] * 2]
    scratch += [(block, BF16), (blocks, BF16), (blocks, F32), (blocks, F32)]
    sems = [pair, (2,), (2,), (2, 2), (UNITS,), pair, pair, (2, UNITS, 3), (7,), (2, 6), (2, UNITS, 3), (2, 2), pair, (UNITS,)]
    return pl.pallas_call(
        main,
        name="main",
        in_specs=[any_spec] * len(args),
        out_specs=[any_spec] * (len(outs) + 1),
        out_shape=[*[like((UNITS, n, *block) if n > 1 else (UNITS, *block), t) for n, t in outs], like(wide, BF16)],
        scratch_shapes=[*[pltpu.VMEM(*one) for one in scratch], *[pltpu.SemaphoreType.DMA(one) for one in sems]],
        compiler_params=pltpu.CompilerParams(collective_id=0, has_side_effects=True, vmem_limit_bytes=VMEM_LIMIT),
        cost_estimate=pl.CostEstimate(flops=34 * T * D * FF, bytes_accessed=600 << 20, transcendentals=3 * T * FF),
    )(*args)


GROUP = 4
PARTS = OWNERS // GROUP


def lay_out(st_ref, m_ref, v_ref, *outs):
    matrix = lax.div(pl.program_id(0), 2 * PARTS)
    moment = W // PARTS

    for number in range(3):
        w_out, m_out, v_out = outs[number::3]

        @pl.when(matrix == number)
        def _():
            for tile in range(4):
                for src, dst in ((st_ref, w_out), (m_ref, m_out), (v_ref, v_out)):
                    rows = W if src is st_ref else moment
                    for o in range(GROUP if src is st_ref else 1):
                        block = src.at[0, tile, 0, o] if src is st_ref else src.at[0, tile, 0]
                        if number == 2:
                            dst[0, o, tile] = block[...]
                        else:
                            for i in range(OWNERS):
                                dst[0, pl.ds(rows * o, rows), pl.ds(512 * i + W * tile, W)] = block[:, pl.ds(W * i, W)]


def run_lay_out(st, mo, vo):
    per = 2 * PARTS
    moment = W // PARTS

    def at(number, s):
        own = jnp.clip(s - number * per, 0, per - 1)
        return lax.div(own, PARTS), lax.rem(own, PARTS)

    def source(s):
        number, own = lax.div(s, per), lax.rem(s, per)
        return 1 - lax.div(own, PARTS), lax.rem(number + 1, 3), lax.rem(own, PARTS)

    def into(s):
        layer, matrix, part = source(s)
        return layer, 0, matrix, part, 0, 0

    def moments_into(s):
        layer, matrix, part = source(s)
        return layer, 0, matrix, part, 0

    like = jax.ShapeDtypeStruct
    specs, shapes = [], []
    for rows, kind in ((GROUP, BF16), (1, F32), (1, F32)):
        for number in range(3):
            height = W if kind == BF16 else moment
            if number == 2:
                block, whole = (1, rows, 4, height, D), (2, OWNERS if kind == BF16 else 1, 4, W, D)
                where = (lambda s: (*at(2, s), 0, 0, 0)) if kind == BF16 else (lambda s: (at(2, s)[0], 0, 0, at(2, s)[1], 0))
            else:
                block, whole = (1, rows * height, FF), (2, D if kind == BF16 else W, FF)
                where = functools.partial(lambda number, s: (*at(number, s), 0), number)
            specs.append(pl.BlockSpec(block, where))
            shapes.append(like(whole, kind))
    moments = pl.BlockSpec((1, 4, 1, moment, D), moments_into)
    out = pl.pallas_call(
        lay_out,
        name="lay_out",
        grid=(3 * per,),
        in_specs=[pl.BlockSpec((1, 4, 1, GROUP, W, D), into), moments, moments],
        out_specs=specs,
        out_shape=shapes,
        compiler_params=pltpu.CompilerParams(dimension_semantics=("arbitrary",), vmem_limit_bytes=VMEM_LIMIT),
    )(st, mo, vo)
    return [t.reshape(2, -1, t.shape[-1]) for t in out]


def solution(mesh):
    def step(x, dy, w_gate, w_up, w_down, m_gate, m_up, m_down, v_gate, v_up, v_down):
        x, dy = x[0], dy[0]
        st, mo, vo, *_ = run_main(x, dy, w_gate, w_up, w_down, m_gate, m_up, m_down, v_gate, v_up, v_down)
        st = st.reshape(2, 4, 3, OWNERS, W, D)
        mo, vo = (t.reshape(2, 4, 3, W, D) for t in (mo, vo))
        return tuple(run_lay_out(st, mo, vo))

    rows = P(None, "dp", None)
    sequences = P(("rep", "dp"), None, None)
    return jax.shard_map(
        step,
        mesh=mesh,
        in_specs=(sequences, sequences, *[P(None, None, None)] * 3, *[rows] * 6),
        out_specs=(*[P("rep", None, None)] * 3, *[P("rep", "dp", None)] * 6),
        check_vma=False,
    )
```

```python
import functools

import jax
import jax.numpy as jnp
from jax import lax
from jax.experimental import pallas as pl
from jax.experimental.pallas import tpu as pltpu
from jax.sharding import PartitionSpec as P

MESH = pl.DeviceIdType.MESH
T, D, FF = 2048, 1024, 4096
CHIPS = 4
OWNERS = 8
W = 128
TILE = 1024
UNITS = 24
STEPS = 24
TILES = 8
VMEM_LIMIT = 63 << 20
WAYS = (0, 1)
ALONG = ((1,), (1,))
F32, BF16 = jnp.float32, jnp.bfloat16
SUMS = ((10, 16, 20, 12), (13, 21, 24, 18), (19, 26, 32, 22))
STEP = (23, 35, 38, 29)
GATHERS = ((30, 43, 45, 36), (39, 48, 50, 41), (50, 55, 58, 48))
LAST = GATHERS[2][3] + 8 * (UNITS - 1)


def normed(wide):
    return (wide * lax.rsqrt(jnp.mean(wide * wide, -1, keepdims=True) + 1e-6)).astype(BF16)


def dot(a, b, dims=((1,), (0,))):
    return lax.dot_general(a, b, (dims, ((), ())), preferred_element_type=F32)


def main(
    x_hbm, dy_hbm, wg_hbm, wu_hbm, wd_hbm, mg_hbm, mu_hbm, md_hbm, vg_hbm, vu_hbm, vd_hbm,
    st, mo, vo, own, par, in_r, in_l,
    a_v, h_v, dy_v, wg_v, wu_v, wd_v, actt_v, dg_v, du_v, da_v, stage,
    t_own, t_par, t_in, t_out, f_own, f_par, f_r, f_l, f_m, f_v, f_w, n_w, n_m, n_v,
    w_sem, big_sem, x_sem, stage_sem, par_sem, t_sem, out_sem, rs_sem, f_sem, n_sem, ag_sem, fwd_sem, d_send, d_recv,
):
    me = lax.axis_index("dp")
    z, core = lax.div(me, 2), lax.rem(me, 2)
    partner = me + 1 - 2 * core
    ends = (3 - z, z)
    behind = (z, 3 - z)
    ahead = (me + 2, me - 2)
    incoming = (in_r, in_l)
    copy = pltpu.make_async_copy

    def remote(src, dst, send, recv, to):
        return pltpu.make_async_remote_copy(
            src_ref=src, dst_ref=dst, send_sem=send, recv_sem=recv, device_id={"dp": to}, device_id_type=MESH
        )

    barrier = pltpu.get_barrier_semaphore()
    pl.semaphore_signal(barrier, inc=1, device_id={"dp": partner}, device_id_type=MESH)
    for way in WAYS:

        @pl.when(ends[way] >= 1)
        def _():
            pl.semaphore_signal(barrier, inc=1, device_id={"dp": ahead[way]}, device_id_type=MESH)

    def strips(src, dst, sem, row, rows, layer, tile):
        for i in range(OWNERS):
            copy(
                src.at[layer, pl.ds(row, rows), pl.ds(pl.multiple_of(512 * i + W * tile, W), W)],
                dst.at[:, pl.ds(W * i, W)],
                sem,
            ).start()

    def weights_in(layer, tile, slot):
        strips(wg_hbm, wg_v.at[slot], w_sem.at[slot, 0], 0, D, layer, tile)
        strips(wu_hbm, wu_v.at[slot], w_sem.at[slot, 1], 0, D, layer, tile)
        for i in range(OWNERS):
            copy(
                wd_hbm.at[layer, pl.ds(pl.multiple_of(512 * i + W * tile, W), W), :],
                wd_v.at[slot, pl.ds(W * i, W), :],
                w_sem.at[slot, 2],
            ).start()

    def weights_wait(slot):
        for number, w in enumerate((wg_v, wu_v, wd_v)):
            copy(w.at[slot], w.at[slot], w_sem.at[slot, number]).wait()


    def at_block(i):
        return pl.ds(pl.multiple_of(i * W, W), W)

    def live(u):
        return (u >= 0) & (u < UNITS)

    def sends(way, hop):
        return (behind[way] <= hop - 1) & (ends[way] >= 1)

    def sum_begin(u, hop):
        def brought(blocks, sem):
            some = pl.ds(0, blocks)
            remote(own.at[0, some], par.at[0, some], stage_sem.at[0, 1], par_sem.at[sem], partner).wait_recv()

        if hop == 1:
            pl.when(u > 0)(functools.partial(brought, CHIPS, u))
        if hop < 3:
            pl.when(u == 0)(functools.partial(brought, 2, UNITS if hop == 1 else 0))
        for way in WAYS:
            block = z + 4 - hop if way == 0 else z + hop - 4

            @pl.when(sends(way, hop))
            def _():
                copy(own.at[u, block], t_own.at[way], t_sem.at[way, 0]).start()
                copy(par.at[u, block], t_par.at[way], t_sem.at[way, 1]).start()

            if hop > 1:

                @pl.when(sends(way, hop) & (behind[way] >= 1))
                def _():
                    landed = incoming[way].at[u, hop - 2]
                    remote(landed, landed, out_sem.at[way, hop - 1], rs_sem.at[way, u, hop - 2], partner).wait_recv()
                    copy(landed, t_in.at[way], t_sem.at[way, 2]).start()

    def sum_out(way, hop, u):
        return remote(
            t_out.at[way, hop - 1],
            incoming[way].at[u, hop - 1],
            out_sem.at[way, hop - 1],
            rs_sem.at[way, u, hop - 1],
            ahead[way],
        )

    def sum_finish(u, hop):
        for way in WAYS:

            @pl.when(sends(way, hop) & (u >= 1))
            def _():
                sum_out(way, hop, u - 1).wait_send()

            @pl.when(sends(way, hop))
            def _():
                copy(own.at[u, 0], t_own.at[way], t_sem.at[way, 0]).wait()
                copy(par.at[u, 0], t_par.at[way], t_sem.at[way, 1]).wait()

                @pl.when(behind[way] == 0)
                def _():
                    t_out[way, hop - 1] = (t_own[way].astype(F32) + t_par[way].astype(F32)).astype(BF16)

                if hop > 1:

                    @pl.when(behind[way] >= 1)
                    def _():
                        copy(own.at[u, 0], t_in.at[way], t_sem.at[way, 2]).wait()
                        t_out[way, hop - 1] = (
                            t_own[way].astype(F32) + t_par[way].astype(F32) + t_in[way].astype(F32)
                        ).astype(BF16)

                sum_out(way, hop, u).start()

    def kind(u):
        tile = lax.div(u, 3)
        return lax.rem(u, 3), 1 - lax.div(tile, 4), lax.rem(tile, 4)

    def step_begin(u):
        copy(own.at[u, z], f_own, f_sem.at[0]).start()
        copy(par.at[u, z], f_par, f_sem.at[1]).start()
        matrix, layer, tile = kind(u)

        @pl.when(matrix == 0)
        def _():
            copy(md_hbm.at[layer, at_block(tile), :], f_m, f_sem.at[4]).start()
            copy(vd_hbm.at[layer, at_block(tile), :], f_v, f_sem.at[5]).start()
            row = pl.ds(pl.multiple_of(512 * me + W * tile, W), W)
            copy(wd_hbm.at[layer, row, :], f_w, f_sem.at[6]).start()

        for number, (m, v, w) in enumerate(((mg_hbm, vg_hbm, wg_hbm), (mu_hbm, vu_hbm, wu_hbm))):

            @pl.when(matrix == number + 1)
            def _():
                strips(m, f_m, f_sem.at[4], 0, W, layer, tile)
                strips(v, f_v, f_sem.at[5], 0, W, layer, tile)
                strips(w, f_w, f_sem.at[6], pl.multiple_of(W * me, W), W, layer, tile)

        for way, f_in in enumerate((f_r, f_l)):

            @pl.when(behind[way] >= 1)
            def _():
                landed = incoming[way].at[u, 2]
                remote(landed, landed, out_sem.at[way, 2], rs_sem.at[way, u, 2], partner).wait_recv()
                copy(landed, f_in, f_sem.at[2 + way]).start()

    def results(u):
        slot = u & 1
        here = st.at[u, me]
        for way in WAYS:
            yield ends[way] >= 1, remote(n_w.at[slot], here, n_sem.at[slot, way], ag_sem.at[way, u, 0], ahead[way])
        yield None, remote(n_w.at[slot], here, n_sem.at[slot, 2], d_recv.at[u], partner)
        yield None, copy(n_w.at[slot], here, n_sem.at[slot, 3])
        yield None, copy(n_m.at[slot], mo.at[u], n_sem.at[slot, 4])
        yield None, copy(n_v.at[slot], vo.at[u], n_sem.at[slot, 5])

    def results_start(u):
        for condition, c in results(u):
            if condition is None:
                c.start()
            else:
                pl.when(condition)(c.start)

    def results_wait(u):
        for number, (condition, c) in enumerate(results(u)):
            wait = c.wait_send if number < 3 else c.wait
            if condition is None:
                wait()
            else:
                pl.when(condition)(wait)

    def step_finish(u):
        @pl.when(u >= 2)
        def _():
            results_wait(u - 2)

        slot = u & 1
        copy(own.at[u, 0], f_own, f_sem.at[0]).wait()
        copy(par.at[u, 0], f_par, f_sem.at[1]).wait()
        copy(mo.at[u], f_m, f_sem.at[4]).wait()
        copy(vo.at[u], f_v, f_sem.at[5]).wait()
        copy(own.at[u, 0], f_w, f_sem.at[6]).wait()
        for way, f_in in enumerate((f_r, f_l)):

            @pl.when(behind[way] >= 1)
            def _():
                copy(own.at[u, 0], f_in, f_sem.at[2 + way]).wait()

        def update(rows, incoming_sum):
            g = f_own[rows, :].astype(F32) + f_par[rows, :].astype(F32) + incoming_sum
            g = g.astype(BF16).astype(F32)
            m = 0.9 * f_m[rows, :] + 0.1 * g
            v = 0.95 * f_v[rows, :] + 0.05 * g * g
            w = f_w[rows, :].astype(F32)
            n_m[slot, rows, :] = m
            n_v[slot, rows, :] = v
            n_w[slot, rows, :] = (w - 0.02 * (m * lax.rsqrt(v + 1e-8) + 0.1 * w)).astype(BF16)

        def updates(*incoming_sums):
            @pl.loop(0, W // 32)
            def _(r):
                rows = pl.ds(pl.multiple_of(r * 32, 32), 32)
                update(rows, sum(one[rows, :].astype(F32) for one in incoming_sums))

        pl.when(z == 0)(functools.partial(updates, f_l))
        pl.when(z == CHIPS - 1)(functools.partial(updates, f_r))
        pl.when((z > 0) & (z < CHIPS - 1))(functools.partial(updates, f_r, f_l))
        results_start(u)

    def gathered(way, hop, u):
        return st.at[u, me - 2 * (hop - 1) if way == 0 else me + 2 * (hop - 1)]

    def pass_on(way, hop, u):
        block = gathered(way, hop, u)
        return remote(block, block, fwd_sem.at[way, hop - 2], ag_sem.at[way, u, hop - 1], ahead[way])

    def across(way, hop, u):
        block = gathered(way, hop, u)
        return remote(block, block, d_send.at[way, hop - 2], d_recv.at[u], partner)

    def gather(u, hop):
        for way in WAYS:

            @pl.when(behind[way] >= hop - 1)
            def _():
                block = gathered(way, hop, u)
                remote(block, block, d_send.at[way, hop - 2], ag_sem.at[way, u, hop - 2], partner).wait_recv()
                if hop < 4:

                    @pl.when((ends[way] >= 1) & (u >= 1))
                    def _():
                        pass_on(way, hop, u - 1).wait_send()

                    @pl.when(ends[way] >= 1)
                    def _():
                        pass_on(way, hop, u).start()

                @pl.when(u >= 1)
                def _():
                    across(way, hop, u - 1).wait_send()

                across(way, hop, u).start()

    def turn(when, b, later, what, *args):
        late = when[3] + later
        u = jnp.where((b & 7 == late % 8) & (b >= late + 24), (b >> 3) - late // 8, -1)
        for early in range(3):
            u = jnp.where(b == when[early] + later, early, u)
        pl.when(live(u))(lambda: what(u, *args))

    def links(b):
        for hop in (1, 2, 3):
            turn(SUMS[hop - 1], b, 1, sum_finish, hop)
        turn(STEP, b, 1, step_finish)
        turn(SUMS[1], b, 0, sum_begin, 2)
        turn(GATHERS[2], b, 0, gather, 4)
        turn(SUMS[0], b, 0, sum_begin, 1)
        turn(SUMS[2], b, 0, sum_begin, 3)
        turn(GATHERS[1], b, 0, gather, 3)
        turn(GATHERS[0], b, 0, gather, 2)
        turn(STEP, b, 0, step_begin)


    def stage_copies(n):
        slot, u, q = n & 1, n >> 2, n & 3
        stay = copy(stage.at[slot, at_block(core), :], own.at[u, q], stage_sem.at[slot, 0])
        sem = jnp.where((n == 0) | (n == 3), UNITS, u)
        go = remote(stage.at[slot, at_block(1 - core), :], par.at[u, q], stage_sem.at[slot, 1], par_sem.at[sem], partner)
        return stay, go

    def stage_wait(n):
        stay, go = stage_copies(n)
        stay.wait()
        go.wait_send()

    def gradient(tile, matrix, q):
        n = (3 * tile + matrix) * 4 + q
        at = chunk(q, 256)
        if matrix == 0:
            g = dot(actt_v[at, :], dy_v[...])
        else:
            g = dot(a_v[:, at], (dg_v if matrix == 1 else du_v)[...], ((0,), (0,)))
        stage[n & 1] = g.astype(BF16)
        for c in stage_copies(n):
            c.start()

    def chunk(k, rows=512):
        return pl.ds(pl.multiple_of(k * rows, rows), rows)

    half = T // 2

    def x_in(c):
        return copy(x_hbm.at[chunk(c, half), :], du_v.at[chunk(c, half), :], x_sem.at[c])

    def plain_in(tile, slot):
        at = chunk(tile, TILE)
        copy(wg_hbm.at[0, :, at], wg_v.at[slot], w_sem.at[slot, 0]).start()
        copy(wu_hbm.at[0, :, at], wu_v.at[slot], w_sem.at[slot, 1]).start()
        copy(wd_hbm.at[0, at, :], wd_v.at[slot], w_sem.at[slot, 2]).start()

    x_in(0).start()
    plain_in(0, 0)
    x_in(1).start()
    da_v[...] = jnp.zeros_like(da_v)

    def forward(t, carry):
        tile, c = lax.div(t, 2), lax.rem(t, 2)
        slot = lax.rem(tile, 2)

        @pl.when(tile == 0)
        def _():
            x_in(c).wait()
            for r in WAYS:
                rows = chunk(2 * c + r)
                a_v[rows, :] = normed(du_v[rows, :].astype(F32))

        @pl.when(c == 0)
        def _():
            weights_wait(slot)
            pl.when(tile == 2)(copy(dy_hbm, dy_v, big_sem.at[1]).start)
            pl.when(tile < 3)(lambda: plain_in(tile + 1, 1 - slot))
            pl.when(tile == 3)(lambda: weights_in(1, 0, 0))

        rows = chunk(c, half)
        for n in range(4):
            cols = pl.ds(256 * n, 256)
            a = a_v[rows, :]
            gate = dot(a, wg_v[slot, :, cols])
            up = dot(a, wu_v[slot, :, cols])
            dg_v[rows, cols] = (gate * jax.nn.sigmoid(gate) * up).astype(BF16)
        da_v[rows, :] += dot(dg_v[rows, :], wd_v[slot])

        @pl.when(tile == 3)
        def _():
            for r in WAYS:
                rows = chunk(2 * c + r)
                h = (du_v[rows, :].astype(F32) + da_v[rows, :].astype(BF16).astype(F32)).astype(BF16)
                h_v[rows, :] = h
                a_v[rows, :] = normed(h.astype(F32))
                da_v[rows, :] = jnp.zeros((512, D), F32)

        return carry

    lax.fori_loop(0, 8, forward, 0)

    def hidden(rows, cols, slot):
        a = a_v[rows, :]
        gate = dot(a, wg_v[slot, :, cols])
        up = dot(a, wu_v[slot, :, cols])
        back = dot(dy_v[rows, :], wd_v[slot, cols, :], ALONG).astype(BF16).astype(F32)
        sig = jax.nn.sigmoid(gate)
        silu = gate * sig
        actt_v[cols, rows] = (silu * up).astype(BF16).T
        du_v[rows, cols] = (back * silu).astype(BF16)
        dg_v[rows, cols] = (back * up * (sig * (1.0 + gate * (1.0 - sig)))).astype(BF16)

    weights_wait(0)
    copy(dy_hbm, dy_v, big_sem.at[1]).wait()
    pl.semaphore_wait(barrier, 1 + (z > 0).astype(jnp.int32) + (z < 3).astype(jnp.int32))

    def first(p, carry):
        inner, c = lax.div(p, 2), lax.rem(p, 2)
        for i in WAYS:
            hidden(chunk(c, half), chunk(inner + i * (3 - 2 * inner), 256), 0)

        @pl.when(p == 2)
        def _():
            stage_wait(0)
            stage_wait(3)

        @pl.when(p >= 2)
        def _():
            links(p + 8)

        @pl.when(c == 1)
        def _():
            def one(i, carry):
                gradient(0, 0, 2 * inner + i * (3 - 4 * inner))
                return carry

            lax.fori_loop(0, 2, one, 0)

        return carry

    lax.fori_loop(0, 4, first, 0)
    stage_wait(2)

    def body(t, carry):
        tile, k = lax.div(t, STEPS), lax.rem(t, STEPS)
        slot = lax.rem(tile, 2)

        @pl.when(k == 0)
        def _():
            weights_wait(slot)

            @pl.when(tile == 4)
            def _():
                copy(x_hbm, a_v, big_sem.at[0]).wait()
                for c in range(4):
                    a_v[chunk(c), :] = normed(a_v[chunk(c), :].astype(F32))

        @pl.when(k < 8)
        def _():
            hidden(chunk(lax.div(k, 2)), chunk(lax.rem(k, 2)), slot)

        pl.when(((k == 8) & (tile < 7)) | (t == 12))(
            lambda: weights_in(1 - lax.div(tile + 1, 4), lax.rem(tile + 1, 4), 1 - slot)
        )

        for matrix in range(3):
            pl.when((k >= 8 + 4 * matrix) & (k < 12 + 4 * matrix))(
                functools.partial(gradient, tile, matrix, k - 8 - 4 * matrix)
            )

        pl.when((k == 20) & (tile == 3))(copy(x_hbm, a_v, big_sem.at[0]).start)

        @pl.when((k >= 20) & (tile < 4))
        def _():
            rows = chunk(k - 20)
            da_v[rows, :] += dot(dg_v[rows, :], wg_v[slot], ALONG) + dot(du_v[rows, :], wu_v[slot], ALONG)

        @pl.when((k >= 20) & (tile == 3))
        def _():
            @pl.loop(0, 4)
            def _(r):
                rows = pl.ds(pl.multiple_of((k - 20) * 512 + r * W, W), W)
                wide = h_v[rows, :].astype(F32)
                da = da_v[rows, :].astype(BF16).astype(F32)
                scale = lax.rsqrt(jnp.mean(wide * wide, -1, keepdims=True) + 1e-6)
                along = jnp.sum(da * wide, -1, keepdims=True) * (scale * scale * scale) * (1.0 / D)
                dh = (da * scale - wide * along).astype(BF16)
                dy_v[rows, :] = (dy_v[rows, :].astype(F32) + dh.astype(F32)).astype(BF16)

        @pl.when((k >= 9) & (k < 21))
        def _():
            stage_wait(jnp.where(t == 12, 1, 12 * tile + k - 9))

        links(t)
        return carry

    lax.fori_loop(12, TILES * STEPS, body, 0)

    def rest(b, carry):
        links(b)
        return carry

    lax.fori_loop(TILES * STEPS, LAST + 1, rest, 0)

    last = UNITS - 1
    for way in WAYS:
        for hop in (1, 2, 3):
            pl.when(sends(way, hop))(sum_out(way, hop, last).wait_send)
        for hop in (2, 3, 4):

            @pl.when(behind[way] >= hop - 1)
            def _():
                if hop < 4:
                    pl.when(ends[way] >= 1)(pass_on(way, hop, last).wait_send)
                across(way, hop, last).wait_send()

    results_wait(last - 1)
    results_wait(last)

    def arrived(u, carry):
        remote(own.at[u], par.at[u], d_send.at[0, 0], d_recv.at[u], partner).wait_recv()
        return carry

    lax.fori_loop(0, UNITS, arrived, 0)


def run_main(*args):
    like = jax.ShapeDtypeStruct
    any_spec = pl.BlockSpec(memory_space=pl.ANY)
    block = (W, D)
    outs = [(OWNERS, BF16), (1, F32), (1, F32), (CHIPS, BF16), (CHIPS, BF16), (3, BF16), (3, BF16)]
    wide, deep, blocks, pair = (T, D), (D, T), (2, *block), (2, 3)
    scratch = [*[(wide, BF16)] * 3, *[((2, D, TILE), BF16)] * 3, (deep, BF16), *[(wide, BF16)] * 2, (wide, F32)]
    scratch += [((2, 256, D), BF16), *[(blocks, BF16)] * 3, ((2, 3, *block), BF16), *[(block, BF16)] * 4, *[(block, F32)] * 2]
    scratch += [(block, BF16), (blocks, BF16), (blocks, F32), (blocks, F32)]
    sems = [pair, (2,), (2,), (2, 2), (UNITS + 1,), pair, pair, (2, UNITS, 3), (7,), (2, 6), (2, UNITS, 3), (2, 2), pair, (UNITS,)]
    return pl.pallas_call(
        main,
        name="main",
        in_specs=[any_spec] * len(args),
        out_specs=[any_spec] * len(outs),
        out_shape=[like((UNITS, n, *block) if n > 1 else (UNITS, *block), t) for n, t in outs],
        scratch_shapes=[*[pltpu.VMEM(*one) for one in scratch], *[pltpu.SemaphoreType.DMA(one) for one in sems]],
        compiler_params=pltpu.CompilerParams(collective_id=0, has_side_effects=True, vmem_limit_bytes=VMEM_LIMIT),
        cost_estimate=pl.CostEstimate(flops=34 * T * D * FF, bytes_accessed=600 << 20, transcendentals=3 * T * FF),
    )(*args)


GROUP = 4
PARTS = OWNERS // GROUP


def lay_out(st_ref, m_ref, v_ref, *outs):
    matrix = lax.div(pl.program_id(0), 2 * PARTS)
    moment = W // PARTS

    for number in range(3):
        w_out, m_out, v_out = outs[number::3]

        @pl.when(matrix == number)
        def _():
            for tile in range(4):
                for src, dst in ((st_ref, w_out), (m_ref, m_out), (v_ref, v_out)):
                    rows = W if src is st_ref else moment
                    for o in range(GROUP if src is st_ref else 1):
                        block = src.at[0, tile, 0, o] if src is st_ref else src.at[0, tile, 0]
                        if number == 2:
                            dst[0, o, tile] = block[...]
                        else:
                            for i in range(OWNERS):
                                dst[0, pl.ds(rows * o, rows), pl.ds(512 * i + W * tile, W)] = block[:, pl.ds(W * i, W)]


def run_lay_out(st, mo, vo):
    per = 2 * PARTS
    moment = W // PARTS

    def at(number, s):
        own = jnp.clip(s - number * per, 0, per - 1)
        return lax.div(own, PARTS), lax.rem(own, PARTS)

    def source(s):
        number, own = lax.div(s, per), lax.rem(s, per)
        return 1 - lax.div(own, PARTS), lax.rem(number + 1, 3), lax.rem(own, PARTS)

    def into(s):
        layer, matrix, part = source(s)
        return layer, 0, matrix, part, 0, 0

    def moments_into(s):
        layer, matrix, part = source(s)
        return layer, 0, matrix, part, 0

    like = jax.ShapeDtypeStruct
    specs, shapes = [], []
    for rows, kind in ((GROUP, BF16), (1, F32), (1, F32)):
        for number in range(3):
            height = W if kind == BF16 else moment
            if number == 2:
                block, whole = (1, rows, 4, height, D), (2, OWNERS if kind == BF16 else 1, 4, W, D)
                where = (lambda s: (*at(2, s), 0, 0, 0)) if kind == BF16 else (lambda s: (at(2, s)[0], 0, 0, at(2, s)[1], 0))
            else:
                block, whole = (1, rows * height, FF), (2, D if kind == BF16 else W, FF)
                where = functools.partial(lambda number, s: (*at(number, s), 0), number)
            specs.append(pl.BlockSpec(block, where))
            shapes.append(like(whole, kind))
    moments = pl.BlockSpec((1, 4, 1, moment, D), moments_into)
    out = pl.pallas_call(
        lay_out,
        name="lay_out",
        grid=(3 * per,),
        in_specs=[pl.BlockSpec((1, 4, 1, GROUP, W, D), into), moments, moments],
        out_specs=specs,
        out_shape=shapes,
        compiler_params=pltpu.CompilerParams(dimension_semantics=("arbitrary",), vmem_limit_bytes=VMEM_LIMIT),
    )(st, mo, vo)
    return [t.reshape(2, -1, t.shape[-1]) for t in out]


def solution(mesh):
    def step(x, dy, w_gate, w_up, w_down, m_gate, m_up, m_down, v_gate, v_up, v_down):
        x, dy = x[0], dy[0]
        st, mo, vo, *_ = run_main(x, dy, w_gate, w_up, w_down, m_gate, m_up, m_down, v_gate, v_up, v_down)
        st = st.reshape(2, 4, 3, OWNERS, W, D)
        mo, vo = (t.reshape(2, 4, 3, W, D) for t in (mo, vo))
        return tuple(run_lay_out(st, mo, vo))

    rows = P(None, "dp", None)
    sequences = P(("rep", "dp"), None, None)
    return jax.shard_map(
        step,
        mesh=mesh,
        in_specs=(sequences, sequences, *[P(None, None, None)] * 3, *[rows] * 6),
        out_specs=(*[P("rep", None, None)] * 3, *[P("rep", "dp", None)] * 6),
        check_vma=False,
    )
```

```python
import functools

import jax
import jax.numpy as jnp
from jax import lax
from jax.experimental import pallas as pl
from jax.experimental.pallas import tpu as pltpu
from jax.sharding import PartitionSpec as P

MESH = pl.DeviceIdType.MESH
T, D, FF = 2048, 1024, 4096
CHIPS = 4
OWNERS = 8
W = 128
TILE = 1024
UNITS = 24
STEPS = 24
TILES = 8
VMEM_LIMIT = 63 << 20
HOPS = (1, 2, 3)
WAYS = (0, 1)
ALONG = ((1,), (1,))
F32, BF16 = jnp.float32, jnp.bfloat16
EARLY = 4
SUMS = ((10, 16, 22, 38, 12), (13, 20, 26, 43, 18), (19, 25, 33, 48, 24))
STEP = (23, 30, 41, 53, 30)
GATHERS = ((28, 38, 48, 59, 37), (39, 44, 52, 67, 42), (46, 51, 62, 73, 51))
LAST = GATHERS[2][EARLY] + 8 * (UNITS - 1)


def normed(wide):
    return (wide * lax.rsqrt(jnp.mean(wide * wide, -1, keepdims=True) + 1e-6)).astype(BF16)


def dot(a, b, dims=((1,), (0,))):
    return lax.dot_general(a, b, (dims, ((), ())), preferred_element_type=F32)


def main(
    x_hbm, dy_hbm, wg_hbm, wu_hbm, wd_hbm, mg_hbm, mu_hbm, md_hbm, vg_hbm, vu_hbm, vd_hbm,
    st, mo, vo, own, par, in_r, in_l,
    a_v, h_v, dy_v, wg_v, wu_v, wd_v, actt_v, dg_v, du_v, da_v, stage,
    t_own, t_par, t_in, t_out, f_own, f_par, f_r, f_l, f_m, f_v, f_w, n_w, n_m, n_v,
    w_sem, big_sem, x_sem, stage_sem, par_sem, t_sem, out_sem, rs_sem, f_sem, n_sem, ag_sem, fwd_sem, d_send, d_recv,
):
    me = lax.axis_index("dp")
    z, core = lax.div(me, 2), lax.rem(me, 2)
    partner = me + 1 - 2 * core
    ends = (3 - z, z)
    behind = (z, 3 - z)
    ahead = (me + 2, me - 2)
    incoming = (in_r, in_l)
    copy = pltpu.make_async_copy

    def remote(src, dst, send, recv, to):
        return pltpu.make_async_remote_copy(
            src_ref=src, dst_ref=dst, send_sem=send, recv_sem=recv, device_id={"dp": to}, device_id_type=MESH
        )

    barrier = pltpu.get_barrier_semaphore()
    pl.semaphore_signal(barrier, inc=1, device_id={"dp": partner}, device_id_type=MESH)
    for way in WAYS:

        @pl.when(ends[way] >= 1)
        def _():
            pl.semaphore_signal(barrier, inc=1, device_id={"dp": ahead[way]}, device_id_type=MESH)

    def strips(src, dst, sem, row, rows, layer, tile):
        for i in range(OWNERS):
            copy(
                src.at[layer, pl.ds(row, rows), pl.ds(pl.multiple_of(512 * i + W * tile, W), W)],
                dst.at[:, pl.ds(W * i, W)],
                sem,
            ).start()

    def weights_in(layer, tile, slot):
        strips(wg_hbm, wg_v.at[slot], w_sem.at[slot, 0], 0, D, layer, tile)
        strips(wu_hbm, wu_v.at[slot], w_sem.at[slot, 1], 0, D, layer, tile)
        for i in range(OWNERS):
            copy(
                wd_hbm.at[layer, pl.ds(pl.multiple_of(512 * i + W * tile, W), W), :],
                wd_v.at[slot, pl.ds(W * i, W), :],
                w_sem.at[slot, 2],
            ).start()

    def weights_wait(slot):
        for number, w in enumerate((wg_v, wu_v, wd_v)):
            copy(w.at[slot], w.at[slot], w_sem.at[slot, number]).wait()


    def at_block(i):
        return pl.ds(pl.multiple_of(i * W, W), W)

    def live(u):
        return (u >= 0) & (u < UNITS)

    def sends(way, hop):
        return (behind[way] <= hop - 1) & (ends[way] >= 1)

    def sum_begin(u, hop):
        def brought(blocks, sem):
            some = pl.ds(0, blocks)
            remote(own.at[0, some], par.at[0, some], stage_sem.at[0, 1], par_sem.at[sem], partner).wait_recv()

        if hop == 1:
            pl.when(u > 0)(functools.partial(brought, CHIPS, u))
        if hop < 3:
            pl.when(u == 0)(functools.partial(brought, 2, UNITS if hop == 1 else 0))
        for way in WAYS:
            block = z + 4 - hop if way == 0 else z + hop - 4

            @pl.when(sends(way, hop))
            def _():
                copy(own.at[u, block], t_own.at[way], t_sem.at[way, 0]).start()
                copy(par.at[u, block], t_par.at[way], t_sem.at[way, 1]).start()

            if hop > 1:

                @pl.when(sends(way, hop) & (behind[way] >= 1))
                def _():
                    landed = incoming[way].at[u, hop - 2]
                    remote(landed, landed, out_sem.at[way, hop - 1], rs_sem.at[way, u, hop - 2], partner).wait_recv()
                    copy(landed, t_in.at[way], t_sem.at[way, 2]).start()

    def sum_out(way, hop, u):
        return remote(
            t_out.at[way, hop - 1],
            incoming[way].at[u, hop - 1],
            out_sem.at[way, hop - 1],
            rs_sem.at[way, u, hop - 1],
            ahead[way],
        )

    def sum_finish(u, hop):
        for way in WAYS:

            @pl.when(sends(way, hop) & (u >= 1))
            def _():
                sum_out(way, hop, u - 1).wait_send()

            @pl.when(sends(way, hop))
            def _():
                copy(own.at[u, 0], t_own.at[way], t_sem.at[way, 0]).wait()
                copy(par.at[u, 0], t_par.at[way], t_sem.at[way, 1]).wait()

                @pl.when(behind[way] == 0)
                def _():
                    t_out[way, hop - 1] = (t_own[way].astype(F32) + t_par[way].astype(F32)).astype(BF16)

                if hop > 1:

                    @pl.when(behind[way] >= 1)
                    def _():
                        copy(own.at[u, 0], t_in.at[way], t_sem.at[way, 2]).wait()
                        t_out[way, hop - 1] = (
                            t_own[way].astype(F32) + t_par[way].astype(F32) + t_in[way].astype(F32)
                        ).astype(BF16)

                sum_out(way, hop, u).start()

    def kind(u):
        tile = lax.div(u, 3)
        return lax.rem(u, 3), 1 - lax.div(tile, 4), lax.rem(tile, 4)

    def step_begin(u):
        copy(own.at[u, z], f_own, f_sem.at[0]).start()
        copy(par.at[u, z], f_par, f_sem.at[1]).start()
        matrix, layer, tile = kind(u)

        @pl.when(matrix == 0)
        def _():
            copy(md_hbm.at[layer, at_block(tile), :], f_m, f_sem.at[4]).start()
            copy(vd_hbm.at[layer, at_block(tile), :], f_v, f_sem.at[5]).start()
            row = pl.ds(pl.multiple_of(512 * me + W * tile, W), W)
            copy(wd_hbm.at[layer, row, :], f_w, f_sem.at[6]).start()

        for number, (m, v, w) in enumerate(((mg_hbm, vg_hbm, wg_hbm), (mu_hbm, vu_hbm, wu_hbm))):

            @pl.when(matrix == number + 1)
            def _():
                strips(m, f_m, f_sem.at[4], 0, W, layer, tile)
                strips(v, f_v, f_sem.at[5], 0, W, layer, tile)
                strips(w, f_w, f_sem.at[6], pl.multiple_of(W * me, W), W, layer, tile)

        for way, f_in in enumerate((f_r, f_l)):

            @pl.when(behind[way] >= 1)
            def _():
                landed = incoming[way].at[u, 2]
                remote(landed, landed, out_sem.at[way, 2], rs_sem.at[way, u, 2], partner).wait_recv()
                copy(landed, f_in, f_sem.at[2 + way]).start()

    def results(u):
        slot = u & 1
        here = st.at[u, me]
        out = [remote(n_w.at[slot], here, n_sem.at[slot, way], ag_sem.at[way, u, 0], ahead[way]) for way in WAYS]
        twin = remote(n_w.at[slot], here, n_sem.at[slot, 2], d_recv.at[u], partner)
        stay = ((n_w, here), (n_m, mo.at[u]), (n_v, vo.at[u]))
        return out, twin, [copy(new.at[slot], to, n_sem.at[slot, 3 + i]) for i, (new, to) in enumerate(stay)]

    def results_start(u):
        out, twin, stay = results(u)
        for way in WAYS:
            pl.when(ends[way] >= 1)(out[way].start)
        for c in (twin, *stay):
            c.start()

    def results_wait(u):
        out, twin, stay = results(u)
        for way in WAYS:
            pl.when(ends[way] >= 1)(out[way].wait_send)
        twin.wait_send()
        for c in stay:
            c.wait()

    def step_finish(u):
        @pl.when(u >= 2)
        def _():
            results_wait(u - 2)

        slot = u & 1
        copy(own.at[u, 0], f_own, f_sem.at[0]).wait()
        copy(par.at[u, 0], f_par, f_sem.at[1]).wait()
        copy(mo.at[u], f_m, f_sem.at[4]).wait()
        copy(vo.at[u], f_v, f_sem.at[5]).wait()
        copy(own.at[u, 0], f_w, f_sem.at[6]).wait()
        for way, f_in in enumerate((f_r, f_l)):

            @pl.when(behind[way] >= 1)
            def _():
                copy(own.at[u, 0], f_in, f_sem.at[2 + way]).wait()

        def update(rows, incoming_sum):
            g = f_own[rows, :].astype(F32) + f_par[rows, :].astype(F32) + incoming_sum
            g = g.astype(BF16).astype(F32)
            m = 0.9 * f_m[rows, :] + 0.1 * g
            v = 0.95 * f_v[rows, :] + 0.05 * g * g
            w = f_w[rows, :].astype(F32)
            n_m[slot, rows, :] = m
            n_v[slot, rows, :] = v
            n_w[slot, rows, :] = (w - 0.02 * (m * lax.rsqrt(v + 1e-8) + 0.1 * w)).astype(BF16)

        def updates(*incoming_sums):
            @pl.loop(0, W // 32)
            def _(r):
                rows = pl.ds(pl.multiple_of(r * 32, 32), 32)
                update(rows, sum(one[rows, :].astype(F32) for one in incoming_sums))

        pl.when(z == 0)(functools.partial(updates, f_l))
        pl.when(z == CHIPS - 1)(functools.partial(updates, f_r))
        pl.when((z > 0) & (z < CHIPS - 1))(functools.partial(updates, f_r, f_l))
        results_start(u)

    def gathered(way, hop, u):
        return st.at[u, me - 2 * (hop - 1) if way == 0 else me + 2 * (hop - 1)]

    def pass_on(way, hop, u):
        block = gathered(way, hop, u)
        return remote(block, block, fwd_sem.at[way, hop - 2], ag_sem.at[way, u, hop - 1], ahead[way])

    def across(way, hop, u):
        block = gathered(way, hop, u)
        return remote(block, block, d_send.at[way, hop - 2], d_recv.at[u], partner)

    def gather(u, hop):
        for way in WAYS:

            @pl.when(behind[way] >= hop - 1)
            def _():
                block = gathered(way, hop, u)
                remote(block, block, d_send.at[way, hop - 2], ag_sem.at[way, u, hop - 2], partner).wait_recv()
                if hop < 4:

                    @pl.when((ends[way] >= 1) & (u >= 1))
                    def _():
                        pass_on(way, hop, u - 1).wait_send()

                    @pl.when(ends[way] >= 1)
                    def _():
                        pass_on(way, hop, u).start()

                @pl.when(u >= 1)
                def _():
                    across(way, hop, u - 1).wait_send()

                across(way, hop, u).start()

    def turn(when, b, what, *args):
        late = when[EARLY]
        u = jnp.where((b & 7 == late % 8) & (b >= late + 8 * EARLY), (b >> 3) - late // 8, -1)
        for early in range(EARLY):
            u = jnp.where(b == when[early], early, u)
        pl.when(live(u))(lambda: what(u, *args))

    def links(b):
        before = b - 1
        for hop in HOPS:
            turn(SUMS[hop - 1], before, sum_finish, hop)
        turn(STEP, before, step_finish)
        turn(STEP, b, step_begin)
        turn(GATHERS[0], b, gather, 2)
        turn(GATHERS[2], b, gather, 4)
        turn(SUMS[1], b, sum_begin, 2)
        turn(GATHERS[1], b, gather, 3)
        turn(SUMS[2], b, sum_begin, 3)
        turn(SUMS[0], b, sum_begin, 1)


    def stage_copies(n):
        slot, u, q = n & 1, n >> 2, n & 3
        stay = copy(stage.at[slot, at_block(core), :], own.at[u, q], stage_sem.at[slot, 0])
        sem = jnp.where((n == 0) | (n == 3), UNITS, u)
        go = remote(stage.at[slot, at_block(1 - core), :], par.at[u, q], stage_sem.at[slot, 1], par_sem.at[sem], partner)
        return stay, go

    def stage_wait(n):
        stay, go = stage_copies(n)
        stay.wait()
        go.wait_send()

    def gradient(tile, matrix, q):
        n = (3 * tile + matrix) * 4 + q
        at = chunk(q, 256)
        if matrix == 0:
            g = dot(actt_v[at, :], dy_v[...])
        else:
            g = dot(a_v[:, at], (dg_v if matrix == 1 else du_v)[...], ((0,), (0,)))
        stage[n & 1] = g.astype(BF16)
        for c in stage_copies(n):
            c.start()

    def chunk(k, rows=512):
        return pl.ds(pl.multiple_of(k * rows, rows), rows)

    half = T // 2

    def x_in(c):
        return copy(x_hbm.at[chunk(c, half), :], du_v.at[chunk(c, half), :], x_sem.at[c])

    def plain_in(tile, slot):
        at = chunk(tile, TILE)
        copy(wg_hbm.at[0, :, at], wg_v.at[slot], w_sem.at[slot, 0]).start()
        copy(wu_hbm.at[0, :, at], wu_v.at[slot], w_sem.at[slot, 1]).start()
        copy(wd_hbm.at[0, at, :], wd_v.at[slot], w_sem.at[slot, 2]).start()

    x_in(0).start()
    plain_in(0, 0)
    x_in(1).start()
    da_v[...] = jnp.zeros_like(da_v)

    def forward(t, carry):
        tile, c = lax.div(t, 2), lax.rem(t, 2)
        slot = lax.rem(tile, 2)

        @pl.when(tile == 0)
        def _():
            x_in(c).wait()
            for r in WAYS:
                rows = chunk(2 * c + r)
                a_v[rows, :] = normed(du_v[rows, :].astype(F32))

        @pl.when(c == 0)
        def _():
            weights_wait(slot)
            pl.when(tile == 2)(copy(dy_hbm, dy_v, big_sem.at[1]).start)
            pl.when(tile < 3)(lambda: plain_in(tile + 1, 1 - slot))
            pl.when(tile == 3)(lambda: weights_in(1, 0, 0))

        rows = chunk(c, half)
        for n in range(4):
            cols = pl.ds(256 * n, 256)
            a = a_v[rows, :]
            gate = dot(a, wg_v[slot, :, cols])
            up = dot(a, wu_v[slot, :, cols])
            dg_v[rows, cols] = (gate * jax.nn.sigmoid(gate) * up).astype(BF16)
        da_v[rows, :] += dot(dg_v[rows, :], wd_v[slot])

        @pl.when(tile == 3)
        def _():
            for r in WAYS:
                rows = chunk(2 * c + r)
                h = (du_v[rows, :].astype(F32) + da_v[rows, :].astype(BF16).astype(F32)).astype(BF16)
                h_v[rows, :] = h
                a_v[rows, :] = normed(h.astype(F32))
                da_v[rows, :] = jnp.zeros((512, D), F32)

        return carry

    lax.fori_loop(0, 8, forward, 0)

    def hidden(rows, cols, slot):
        a = a_v[rows, :]
        gate = dot(a, wg_v[slot, :, cols])
        up = dot(a, wu_v[slot, :, cols])
        back = dot(dy_v[rows, :], wd_v[slot, cols, :], ALONG).astype(BF16).astype(F32)
        sig = jax.nn.sigmoid(gate)
        silu = gate * sig
        actt_v[cols, rows] = (silu * up).astype(BF16).T
        du_v[rows, cols] = (back * silu).astype(BF16)
        dg_v[rows, cols] = (back * up * (sig * (1.0 + gate * (1.0 - sig)))).astype(BF16)

    weights_wait(0)
    copy(dy_hbm, dy_v, big_sem.at[1]).wait()
    pl.semaphore_wait(barrier, 1 + (z > 0).astype(jnp.int32) + (z < 3).astype(jnp.int32))

    def first(p, carry):
        inner, c = lax.div(p, 2), lax.rem(p, 2)
        for i in WAYS:
            hidden(chunk(c, half), chunk(inner + i * (3 - 2 * inner), 256), 0)

        @pl.when(p == 2)
        def _():
            stage_wait(0)
            stage_wait(3)

        @pl.when(p >= 2)
        def _():
            links(p + 8)

        @pl.when(c == 1)
        def _():
            def one(i, carry):
                gradient(0, 0, 2 * inner + i * (3 - 4 * inner))
                return carry

            lax.fori_loop(0, 2, one, 0)

        return carry

    lax.fori_loop(0, 4, first, 0)
    stage_wait(2)

    def body(tile, carry):
        slot = tile & 1
        begun = jnp.where(tile == 0, 1, 0)
        step = tile * STEPS
        chunks = tile * 12

        def steps(first, start, end, what):
            def one(i, carry):
                what(i)
                links(step + first + i)
                return carry

            lax.fori_loop(start, end, one, 0)

        @pl.when(tile > 0)
        def _():
            weights_wait(slot)

        @pl.when(tile == 4)
        def _():
            copy(x_hbm, a_v, big_sem.at[0]).wait()
            for c in range(4):
                a_v[chunk(c), :] = normed(a_v[chunk(c), :].astype(F32))

        steps(0, begun * 8, 8, lambda i: hidden(chunk(i >> 1), chunk(i & 1), slot))

        @pl.when(tile < TILES - 1)
        def _():
            weights_in(1 - ((tile + 1) >> 2), (tile + 1) & 3, 1 - slot)

        def down(q):
            gradient(tile, 0, q)
            pl.when(q > 0)(lambda: stage_wait(chunks + q - 1))

        def gate(q):
            gradient(tile, 1, q)
            stage_wait(jnp.where(tile + q == 0, 1, chunks + q + 3))

        def up(q):
            gradient(tile, 2, q)
            stage_wait(chunks + q + 7)

        def inner(c):
            @pl.when(tile < 4)
            def _():
                rows = chunk(c)
                da_v[rows, :] += dot(dg_v[rows, :], wg_v[slot], ALONG) + dot(du_v[rows, :], wu_v[slot], ALONG)

            @pl.when(tile == 3)
            def _():
                @pl.loop(0, 4)
                def _(r):
                    rows = pl.ds(pl.multiple_of(c * 512 + r * W, W), W)
                    wide = h_v[rows, :].astype(F32)
                    da = da_v[rows, :].astype(BF16).astype(F32)
                    scale = lax.rsqrt(jnp.mean(wide * wide, -1, keepdims=True) + 1e-6)
                    along = jnp.sum(da * wide, -1, keepdims=True) * (scale * scale * scale) * (1.0 / D)
                    dh = (da * scale - wide * along).astype(BF16)
                    dy_v[rows, :] = (dy_v[rows, :].astype(F32) + dh.astype(F32)).astype(BF16)

            pl.when(c == 0)(lambda: stage_wait(chunks + 11))

        steps(8, begun * 4, 4, down)
        steps(12, 0, 4, gate)
        steps(16, 0, 4, up)
        pl.when(tile == 3)(copy(x_hbm, a_v, big_sem.at[0]).start)
        steps(20, 0, 4, inner)
        return carry

    lax.fori_loop(0, TILES, body, 0)

    def rest(b, carry):
        links(b)
        return carry

    lax.fori_loop(TILES * STEPS, LAST + 1, rest, 0)

    last = UNITS - 1
    for way in WAYS:
        for hop in HOPS:
            pl.when(sends(way, hop))(sum_out(way, hop, last).wait_send)
        for hop in (2, 3, 4):

            @pl.when(behind[way] >= hop - 1)
            def _():
                if hop < 4:
                    pl.when(ends[way] >= 1)(pass_on(way, hop, last).wait_send)
                across(way, hop, last).wait_send()

    results_wait(last - 1)
    results_wait(last)

    def arrived(u, carry):
        remote(own.at[u], par.at[u], d_send.at[0, 0], d_recv.at[u], partner).wait_recv()
        return carry

    lax.fori_loop(0, UNITS, arrived, 0)


def run_main(*args):
    like = jax.ShapeDtypeStruct
    any_spec = pl.BlockSpec(memory_space=pl.ANY)
    block = (W, D)
    outs = [(OWNERS, BF16), (1, F32), (1, F32), (CHIPS, BF16), (CHIPS, BF16), (3, BF16), (3, BF16)]
    wide, deep, blocks, pair = (T, D), (D, T), (2, *block), (2, 3)
    scratch = [*[(wide, BF16)] * 3, *[((2, D, TILE), BF16)] * 3, (deep, BF16), *[(wide, BF16)] * 2, (wide, F32)]
    scratch += [((2, 256, D), BF16), *[(blocks, BF16)] * 3, ((2, 3, *block), BF16), *[(block, BF16)] * 4, *[(block, F32)] * 2]
    scratch += [(block, BF16), (blocks, BF16), (blocks, F32), (blocks, F32)]
    sems = [pair, (2,), (2,), (2, 2), (UNITS + 1,), pair, pair, (2, UNITS, 3), (7,), (2, 6), (2, UNITS, 3), (2, 2), pair, (UNITS,)]
    return pl.pallas_call(
        main,
        name="main",
        in_specs=[any_spec] * len(args),
        out_specs=[any_spec] * len(outs),
        out_shape=[like((UNITS, n, *block) if n > 1 else (UNITS, *block), t) for n, t in outs],
        scratch_shapes=[*[pltpu.VMEM(*one) for one in scratch], *[pltpu.SemaphoreType.DMA(one) for one in sems]],
        compiler_params=pltpu.CompilerParams(collective_id=0, has_side_effects=True, vmem_limit_bytes=VMEM_LIMIT),
        cost_estimate=pl.CostEstimate(flops=34 * T * D * FF, bytes_accessed=600 << 20, transcendentals=3 * T * FF),
    )(*args)


GROUP = 4
PARTS = OWNERS // GROUP


def lay_out(st_ref, m_ref, v_ref, *outs):
    matrix = lax.div(pl.program_id(0), 2 * PARTS)
    moment = W // PARTS

    for number in range(3):
        w_out, m_out, v_out = outs[number::3]

        @pl.when(matrix == number)
        def _():
            for tile in range(4):
                for src, dst in ((st_ref, w_out), (m_ref, m_out), (v_ref, v_out)):
                    rows = W if src is st_ref else moment
                    for o in range(GROUP if src is st_ref else 1):
                        block = src.at[0, tile, 0, o] if src is st_ref else src.at[0, tile, 0]
                        if number == 2:
                            dst[0, o, tile] = block[...]
                        else:
                            for i in range(OWNERS):
                                dst[0, pl.ds(rows * o, rows), pl.ds(512 * i + W * tile, W)] = block[:, pl.ds(W * i, W)]


def run_lay_out(st, mo, vo):
    per = 2 * PARTS
    moment = W // PARTS

    def at(number, s):
        own = jnp.clip(s - number * per, 0, per - 1)
        return lax.div(own, PARTS), lax.rem(own, PARTS)

    def source(s):
        number, own = lax.div(s, per), lax.rem(s, per)
        return 1 - lax.div(own, PARTS), lax.rem(number + 1, 3), lax.rem(own, PARTS)

    def into(s):
        layer, matrix, part = source(s)
        return layer, 0, matrix, part, 0, 0

    def moments_into(s):
        layer, matrix, part = source(s)
        return layer, 0, matrix, part, 0

    like = jax.ShapeDtypeStruct
    specs, shapes = [], []
    for rows, kind in ((GROUP, BF16), (1, F32), (1, F32)):
        for number in range(3):
            height = W if kind == BF16 else moment
            if number == 2:
                block, whole = (1, rows, 4, height, D), (2, OWNERS if kind == BF16 else 1, 4, W, D)
                where = (lambda s: (*at(2, s), 0, 0, 0)) if kind == BF16 else (lambda s: (at(2, s)[0], 0, 0, at(2, s)[1], 0))
            else:
                block, whole = (1, rows * height, FF), (2, D if kind == BF16 else W, FF)
                where = functools.partial(lambda number, s: (*at(number, s), 0), number)
            specs.append(pl.BlockSpec(block, where))
            shapes.append(like(whole, kind))
    moments = pl.BlockSpec((1, 4, 1, moment, D), moments_into)
    out = pl.pallas_call(
        lay_out,
        name="lay_out",
        grid=(3 * per,),
        in_specs=[pl.BlockSpec((1, 4, 1, GROUP, W, D), into), moments, moments],
        out_specs=specs,
        out_shape=shapes,
        compiler_params=pltpu.CompilerParams(dimension_semantics=("arbitrary",), vmem_limit_bytes=VMEM_LIMIT),
    )(st, mo, vo)
    return [t.reshape(2, -1, t.shape[-1]) for t in out]


def solution(mesh):
    def step(x, dy, w_gate, w_up, w_down, m_gate, m_up, m_down, v_gate, v_up, v_down):
        x, dy = x[0], dy[0]
        st, mo, vo, *_ = run_main(x, dy, w_gate, w_up, w_down, m_gate, m_up, m_down, v_gate, v_up, v_down)
        st = st.reshape(2, 4, 3, OWNERS, W, D)
        mo, vo = (t.reshape(2, 4, 3, W, D) for t in (mo, vo))
        return tuple(run_lay_out(st, mo, vo))

    rows = P(None, "dp")
    sequences = P(("rep", "dp"))
    return jax.shard_map(
        step,
        mesh=mesh,
        in_specs=(sequences, sequences, *[P()] * 3, *[rows] * 6),
        out_specs=(*[P("rep")] * 3, *[P("rep", "dp")] * 6),
        check_vma=False,
    )
```
